32 devices in a mesh: dp: 8 (over y, x, core), tensor: 4 (over z).
Axes of the slice: x: 2, y: 2, z: 4, core: 2. Of those that a mesh axis runs over, the one named last changes fastest.
Arguments:
- acts: bfloat16 [1024, 4096], P('dp'), may hold values from -6 to 6
- grad_out: bfloat16 [1024, 14336], P('dp', 'tensor'), may hold values from -0.1875 to 0.1875
- selected: int32 [4, 4], P('tensor'), may hold values from 0 to 27, as said below
- owner: int32 [4, 192, 1], P('tensor'), may hold values from 0 to 7; in each aligned block of 192 rows (0 to 191, 192 to 383, ..., all dimensions but the last counted through in order) at most 36 rows name the same one
- sel_weight: float32 [4096, 2048], P('dp', 'tensor'), may hold values from -3 to 3
- sel_moment: float32 [4096, 2048], P('dp', 'tensor'), may hold values from -3 to 3
- sel_second: float32 [4096, 2048], P('dp', 'tensor'), may hold values from 0.01 to 1
- off_weight: float32 [8, 4, 36, 512, 128], P('dp', 'tensor'), may hold values from -3 to 3
- off_moment: float32 [8, 4, 36, 512, 128], P('dp', 'tensor'), may hold values from -3 to 3
- off_second: float32 [8, 4, 36, 512, 128], P('dp', 'tensor'), may hold values from 0.01 to 1
Outputs:
- column_norm: float32 [14336], P('tensor')
- sel_weight_new: float32 [4096, 2048], P('dp', 'tensor')
- sel_moment_new: float32 [4096, 2048], P('dp', 'tensor')
- sel_second_new: float32 [4096, 2048], P('dp', 'tensor')
- off_weight_new: float32 [8, 4, 36, 512, 128], P('dp', 'tensor')
- off_moment_new: float32 [8, 4, 36, 512, 128], P('dp', 'tensor')
- off_second_new: float32 [8, 4, 36, 512, 128], P('dp', 'tensor')
The draws below stay inside these ranges and needn't reach their ends.
Inputs may be any that keep to these rules, and one draw needn't show every extreme that they name: `selected`: each row names 4 tile. For each index of tensor, no owner receives more than 36 pieces, and some owner receives exactly 36.
All inputs are finite; a program needn't handle non-finite values.
Results may differ from the reference program's by a relative error of at most 0.0017.
Values may be sent and summed in bfloat16 or wider, within the bound.
A program may use at most 192 MiB of HBM per device.

```python
import math
import jax
import jax.numpy as jnp
import numpy as np
from jax import lax

ROWS = 4096
FFW = 14336
TILE = 128
TOK_DEV = 128
TOKENS = 1024
TILES_DEV = 28
SEL_TILES = 4
REST_TILES = 24
BLOCK_ROWS = 512
PIECES = 192
CAP = 36
N_DP = 8
N_TENSOR = 4


def draw_selected(key, part):
    row_keys = jax.random.split(jax.random.fold_in(key, 17), N_TENSOR)
    shuffled = jax.vmap(lambda row_key: jax.random.permutation(row_key, TILES_DEV))(row_keys)
    return jnp.sort(shuffled[:, :SEL_TILES], axis=1).astype(jnp.int32)


def shard_levels(key, extent, cuts, low, high):
    def one(axis_at, parts):
        heights = jax.random.uniform(jax.random.fold_in(jax.random.fold_in(key, 6), axis_at), (parts,), jnp.float32, low / len(cuts), high / len(cuts))
        return jnp.repeat(jnp.exp(heights), extent[axis_at] // parts).reshape((-1,) + (1,) * (len(extent) - axis_at - 1))

    factor_of = one(*cuts[0])
    for cut in cuts[1:]:
        factor_of = factor_of * one(*cut)
    return factor_of


def deal_out(own_key, own, number, rows, amount, top, bound, slope):
    order = jax.random.permutation(own_key, amount)
    crowded, usual = shares(amount, rows * top, bound, slope, True), shares(amount, rows * top, bound, slope, False)
    places = jnp.arange(amount)

    def named(lengths, rotation):
        used = int((lengths > 0).sum())
        fixed = max(1, used // 4)
        shifted = fixed + (places - fixed + rotation * (used - fixed)) % max(1, amount - fixed)
        return jnp.zeros((amount,), jnp.int32).at[order[jnp.where(places < fixed, places, shifted)]].set(jnp.asarray(lengths, jnp.int32))

    lengths = jnp.where(number % 4 == 0, named(crowded, number // 4), named(usual, number - number // 4 - 1))
    mixed = jax.random.permutation(jax.random.fold_in(own, 3), amount)
    giver, receiver = mixed[0:amount // 2 * 2:2], mixed[1:amount // 2 * 2:2]
    slack = jnp.minimum(lengths[giver] - 1, bound - lengths[receiver]) // 2
    slack = jnp.where((giver == order[0]) | (receiver == order[0]) | (lengths[receiver] == 0), 0, jnp.maximum(slack, 0))
    shifted = jax.random.randint(jax.random.fold_in(own, 4), (amount // 2,), 0, 1 << 20) % (slack + 1)
    lengths = lengths.at[giver].add(-shifted).at[receiver].add(shifted)
    members = jnp.searchsorted(jnp.cumsum(lengths), jnp.arange(rows * top), side="right").astype(jnp.int32)
    table = members.reshape(top, rows).T
    table = table[jax.random.permutation(jax.random.fold_in(own, 1), rows)]
    rotation = jax.random.randint(jax.random.fold_in(own, 2), (rows, 1), 0, top)
    return jnp.take_along_axis(table, (jnp.arange(top)[None, :] + rotation) % top, axis=1)


def shares(amount, total, bound, skew, full):
    loads = [(1 << 20) // math.isqrt(grade ** skew) + 1 for grade in range(1, amount + 1)]
    largest = bound if full else min(bound, max(-(-total // amount), total * loads[0] // sum(loads)))
    least = 1 if total - largest >= amount - 1 else 0
    given, rest = [largest] + [least] * (amount - 1), total - largest - least * (amount - 1)
    while rest > 0:
        movable = [i for i in range(1, amount) if given[i] < largest] or [i for i in range(1, amount) if given[i] < bound]
        whole, left = sum([loads[i] for i in movable]), rest
        for i in movable:
            extra = min(bound - given[i], max(1, left * loads[i] // whole), rest)
            given[i] = given[i] + extra
            rest = rest - extra
    return np.array(given)


def centred(rng, dims, deviation, bound, cuts=(), kind=jnp.bfloat16):
    entries = deviation * jax.random.normal(rng, dims, jnp.float32)
    if cuts:
        entries = entries * shard_levels(rng, dims, cuts, -0.22, 0.18)
    return jnp.clip(entries, -bound, bound).astype(kind)


def setup_inputs(seed: int = 0) -> dict:
    keys = jax.random.split(jax.random.key(seed), 11)
    acts = centred(keys[0], (TOKENS, ROWS), 1.0, 6.0, ((0, 8),))
    grad_out = centred(keys[1], (TOKENS, FFW), TOKENS ** -0.5, 0.1875, ((0, 8), (1, 4)))
    selected = draw_selected(jax.random.fold_in(keys[10], 71), 0)
    owner_keys = jax.random.split(jax.random.fold_in(keys[3], 1), N_TENSOR * PIECES // PIECES)
    owner_turns = jax.random.permutation(jax.random.fold_in(keys[3], 3), N_TENSOR * PIECES // PIECES)
    owner = jax.vmap(lambda own, number: deal_out(jax.random.fold_in(keys[3], 2), own, number, PIECES, N_DP, 1, CAP, 2))(owner_keys, owner_turns).reshape((N_TENSOR, PIECES, 1))
    sel_weight = centred(keys[4], (ROWS, N_TENSOR * SEL_TILES * TILE), 0.5, 3.0, ((0, 8), (1, 4)), jnp.float32)
    sel_moment = centred(keys[5], (ROWS, N_TENSOR * SEL_TILES * TILE), 0.5, 3.0, ((0, 8), (1, 4)), jnp.float32)
    sel_second = jnp.clip(jnp.exp(math.log(1.0) - 4.6051702 * jax.random.uniform(keys[6], (ROWS, N_TENSOR * SEL_TILES * TILE), jnp.float32) ** shard_levels(keys[6], (ROWS, N_TENSOR * SEL_TILES * TILE), ((0, 8), (1, 4)), -0.2, 0.2)), 0.01, 1.0)
    off_weight = centred(keys[7], (N_DP, N_TENSOR, CAP, BLOCK_ROWS, TILE), 0.5, 3.0, ((0, 8), (1, 4)), jnp.float32)
    off_moment = centred(keys[8], (N_DP, N_TENSOR, CAP, BLOCK_ROWS, TILE), 0.5, 3.0, ((0, 8), (1, 4)), jnp.float32)
    off_second = jnp.clip(jnp.exp(math.log(1.0) - 4.6051702 * jax.random.uniform(keys[9], (N_DP, N_TENSOR, CAP, BLOCK_ROWS, TILE), jnp.float32) ** shard_levels(keys[9], (N_DP, N_TENSOR, CAP, BLOCK_ROWS, TILE), ((0, 8), (1, 4)), -0.2, 0.2)), 0.01, 1.0)
    return dict(acts=acts, grad_out=grad_out, selected=selected, owner=owner, sel_weight=sel_weight, sel_moment=sel_moment, sel_second=sel_second, off_weight=off_weight, off_moment=off_moment, off_second=off_second)


beta_one = 0.9
beta_two = 0.95
adam_eps = 1e-08
learn_rate = 0.01
decay_rate = 0.1
step_count = 10.0

def adam_update(weight, moment, second, grad):
    moment_new = beta_one * moment + (1.0 - beta_one) * grad
    second_new = beta_two * second + (1.0 - beta_two) * grad * grad
    first_fix = 1.0 - beta_one ** step_count
    second_fix = 1.0 - beta_two ** step_count
    update = moment_new / first_fix / (jnp.sqrt(second_new / second_fix) + adam_eps)
    return (weight - learn_rate * (update + decay_rate * weight), moment_new, second_new)

def rest_tiles(selected_row):
    tiles = jnp.arange(TILES_DEV, dtype=jnp.int32)
    chosen = jnp.any(tiles[:, None] == selected_row[None, :], axis=1).astype(jnp.int32)
    order = jnp.argsort(chosen * TILES_DEV + tiles).astype(jnp.int32)
    return order[:REST_TILES]

def slot_numbers(owner_row):
    places = jnp.arange(owner_row.shape[0], dtype=jnp.int32)
    earlier = (owner_row[:, None] == owner_row[None, :]) & (places[:, None] > places[None, :])
    return lax.optimization_barrier(jnp.sum(earlier.astype(jnp.int32), axis=1)).astype(jnp.int32)

def place_pieces(piece_row, owner_row):
    target = (owner_row * CAP + slot_numbers(owner_row)).astype(jnp.int32)
    empty = jnp.zeros((N_DP * CAP, BLOCK_ROWS, TILE), jnp.bfloat16)
    return empty.at[target].set(piece_row).reshape(N_DP, CAP, BLOCK_ROWS, TILE)

def reference(acts, grad_out, selected, owner, sel_weight, sel_moment, sel_second, off_weight, off_moment, off_second):
    rest_lists = jax.vmap(rest_tiles)(selected)
    acts_shards = acts.reshape(N_DP, TOK_DEV, ROWS)
    grad_shards = grad_out.reshape(N_DP, TOK_DEV, FFW)
    sel_index = selected.astype(jnp.int32)[None, :, :, None]
    rest_index = rest_lists.astype(jnp.int32)[None, :, :, None]

    def add_shard(carry, shard):
        squares, sel_sum, rest_sum = carry
        partial_value = jnp.dot(shard[0].T, shard[1], preferred_element_type=jnp.float32)
        squares = squares + lax.optimization_barrier(jnp.sum(partial_value * partial_value, axis=0))
        tiled = partial_value.reshape(ROWS, N_TENSOR, TILES_DEV, TILE)
        sel_part = jnp.take_along_axis(tiled, sel_index, axis=2).reshape(ROWS, N_TENSOR * SEL_TILES * TILE)
        rest_part = jnp.take_along_axis(tiled, rest_index, axis=2).astype(jnp.bfloat16)
        rest_part = lax.optimization_barrier(rest_part).astype(jnp.float32)
        return ((squares, sel_sum + sel_part, rest_sum + rest_part), None)
    start = (jnp.zeros((FFW,), jnp.float32), jnp.zeros((ROWS, N_TENSOR * SEL_TILES * TILE), jnp.float32), jnp.zeros((ROWS, N_TENSOR, REST_TILES, TILE), jnp.float32))
    (squares, sel_sum, rest_sum), unused = lax.scan(add_shard, start, (acts_shards, grad_shards))
    column_norm = jnp.sqrt(squares)
    new_sel = adam_update(sel_weight, sel_moment, sel_second, sel_sum)
    pieces = rest_sum.astype(jnp.bfloat16).reshape(N_DP, BLOCK_ROWS, N_TENSOR, REST_TILES, TILE)
    pieces = jnp.transpose(pieces, (2, 3, 0, 1, 4)).reshape(N_TENSOR, PIECES, BLOCK_ROWS, TILE)
    slots = jax.vmap(place_pieces)(pieces, owner[:, :, 0].astype(jnp.int32))
    offload = jnp.transpose(slots, (1, 0, 2, 3, 4)).astype(jnp.float32)
    new_off = adam_update(off_weight, off_moment, off_second, offload)
    return (column_norm, new_sel[0], new_sel[1], new_sel[2], new_off[0], new_off[1], new_off[2])
```

```python
import functools

import jax
import jax.numpy as jnp
from jax import lax
from jax.experimental import pallas as pl
from jax.experimental.pallas import tpu as pltpu
from jax.sharding import PartitionSpec as P

TILE = 128
VMEM_LIMIT = 56 * 1024 * 1024


beta_one = 0.9
beta_two = 0.95
adam_eps = 1e-08
learn_rate = 0.01
decay_rate = 0.1
step_count = 10.0


def adam_update(weight, moment, second, grad):
    moment_new = beta_one * moment + (1.0 - beta_one) * grad
    second_new = beta_two * second + (1.0 - beta_two) * grad * grad
    first_fix = 1.0 - beta_one**step_count
    second_fix = 1.0 - beta_two**step_count
    update = moment_new / first_fix / (jnp.sqrt(second_new / second_fix) + adam_eps)
    return (weight - learn_rate * (update + decay_rate * weight), moment_new, second_new)


MESH = pl.DeviceIdType.MESH


def flip_bits(index, mask):
    result, bit = index, 1
    while bit <= mask:
        if mask & bit:
            result = result + bit * (1 - 2 * ((index // bit) % 2))
        bit *= 2
    return result


def gather_kernel(
    n,
    tile_slot,
    block_slot,
    sel_tile,
    acts,
    acts_t,
    grad,
    offload,
    sel_sum,
    norm,
    total,
    squares,
    send_sem,
    recv_a,
    recv_g,
    send_q,
    recv_q,
    *held,
):
    held_a, held_g = (acts_t,) + held[: n - 1], (grad,) + held[n - 1 :]
    me = lax.axis_index("dp")
    capacity = offload.shape[0]
    sel_count = sel_tile.shape[0]
    rows_all = acts.shape[1]

    barrier = pltpu.get_barrier_semaphore()
    for mask in range(1, n):
        pl.semaphore_signal(
            barrier, inc=1, device_id={"dp": flip_bits(me, mask)}, device_id_type=MESH
        )
    pl.semaphore_wait(barrier, n - 1)

    started = []

    def block_of(kind, mask):
        return (held_a if kind == "a" else held_g)[mask]

    def copy_of(kind, mask, peer, number):
        there = mask ^ peer
        return pltpu.make_async_remote_copy(
            src_ref=block_of(kind, mask),
            dst_ref=block_of(kind, there),
            send_sem=send_sem.at[number],
            recv_sem=(recv_a if kind == "a" else recv_g).at[there - 1],
            device_id={"dp": flip_bits(me, peer)},
            device_id_type=MESH,
        )

    def send(kind, mask, peer):
        copy = copy_of(kind, mask, peer, len(started))
        copy.start()
        started.append(copy)

    def arrived(kind, mask):
        copy_of(kind, 0, mask, 0).wait_recv()

    def square_columns():
        gram = jnp.dot(
            acts[...], acts_t[...].reshape(rows_all, -1), preferred_element_type=jnp.float32
        )
        high = gram.astype(jnp.bfloat16)
        rest = gram - high.astype(jnp.float32)
        middle = rest.astype(jnp.bfloat16)
        low = (rest - middle.astype(jnp.float32)).astype(jnp.bfloat16)

        @pl.loop(0, grad.shape[0])
        def _(tile):
            piece = grad[tile]
            product = jnp.dot(low, piece, preferred_element_type=jnp.float32)
            product += jnp.dot(middle, piece, preferred_element_type=jnp.float32)
            product += jnp.dot(high, piece, preferred_element_type=jnp.float32)
            squares[0, tile] = jnp.sum(
                piece.astype(jnp.float32) * product, axis=0, keepdims=True
            )

    def square_copy(mask):
        return pltpu.make_async_remote_copy(
            src_ref=squares.at[0],
            dst_ref=squares.at[mask],
            send_sem=send_q.at[mask - 1],
            recv_sem=recv_q.at[mask - 1],
            device_id={"dp": flip_bits(me, mask)},
            device_id_type=MESH,
        )

    def add_blocks(masks, first, last):
        def product(mask, block, tile):
            return jnp.dot(
                held_a[mask][block], held_g[mask][tile], preferred_element_type=jnp.float32
            )

        @pl.loop(0, capacity)
        def _(slot):
            block, tile = block_slot[slot], tile_slot[slot]
            value = None if first else total[slot]
            for mask in masks:
                part = product(mask, block, tile)
                part = part.astype(jnp.bfloat16).astype(jnp.float32)
                value = part if value is None else value + part
            if last:
                offload[slot] = value.astype(jnp.bfloat16)
            else:
                total[slot] = value

        for i in range(sel_count):
            tile = sel_tile[i]
            place = pl.ds(i * TILE, TILE)
            value = None if first else sel_sum[:, place]
            for mask in masks:
                part = product(mask, me, tile)
                value = part if value is None else value + part
            sel_sum[:, place] = value

    if n == 8:
        core, near, far = 1, 2, 4
        send("g", 0, near)
        send("a", 0, far)
        send("a", 0, core)
        send("g", 0, core)
        send("a", 0, near)
        send("g", 0, far)
        square_columns()
        arrived("a", core)
        arrived("g", core)
        add_blocks((0, core), True, False)
        for mask in range(1, n):
            square_copy(mask).start()
        arrived("g", near)
        send("g", near, far)
        send("g", near, core)
        arrived("a", far)
        send("a", far, near)
        send("a", far, core)
        arrived("a", near)
        send("a", near, core)
        arrived("g", far)
        send("g", far, core)
        for mask in (near, far):
            arrived("a", mask ^ core)
            arrived("g", mask ^ core)
        add_blocks((near, near ^ core, far, far ^ core), False, False)
        both = near ^ far
        arrived("a", both)
        send("a", both, core)
        arrived("g", both)
        send("g", both, core)
        arrived("a", both ^ core)
        arrived("g", both ^ core)
        add_blocks((both, both ^ core), False, True)
    else:
        for mask in range(1, n):
            send("g", 0, mask)
            send("a", 0, mask)
        square_columns()
        add_blocks((0,), True, False)
        for mask in range(1, n):
            square_copy(mask).start()
        for mask in range(1, n):
            arrived("a", mask)
            arrived("g", mask)
            add_blocks((mask,), False, mask == n - 1)

    whole = squares[0]
    for mask in range(1, n):
        square_copy(mask).wait_recv()
        whole = whole + squares[mask]
    norm[...] = jnp.sqrt(whole)
    for copy in started:
        copy.wait_send()
    for mask in range(1, n):
        square_copy(mask).wait_send()


def body(
    acts,
    grad_out,
    selected,
    owner,
    sel_weight,
    sel_moment,
    sel_second,
    off_weight,
    off_moment,
    off_second,
):
    n = lax.axis_size("dp")
    tokens_here, rows_all = acts.shape
    cols_here = grad_out.shape[1]
    tiles_here = cols_here // TILE
    sel_count = selected.shape[1]
    rest_count = tiles_here - sel_count
    row_block = rows_all // n
    capacity = off_weight.shape[2]
    piece_count = rest_count * n
    selected_row = selected[0]
    owner_row = owner[0, :, 0]
    mine = (owner_row == lax.axis_index("dp")).astype(jnp.int32)
    pieces = jnp.arange(piece_count, dtype=jnp.int32)
    before = jnp.sum(mine[None, :] * (pieces[:, None] > pieces[None, :]), axis=1)
    taken = mine[None, :] * (before[None, :] == jnp.arange(capacity)[:, None])
    piece = jnp.sum(taken * pieces[None, :], axis=1)
    filled = jnp.sum(taken, axis=1) > 0
    order = piece // n
    tiles = jnp.arange(tiles_here, dtype=jnp.int32)
    free = 1 - jnp.any(tiles[:, None] == selected_row[None, :], axis=1).astype(jnp.int32)
    rank = jnp.sum(free[None, :] * (tiles[:, None] > tiles[None, :]), axis=1)
    named = free[None, :] * (rank[None, :] == order[:, None])
    tile_slot = jnp.sum(named * tiles[None, :], axis=1).astype(jnp.int32)
    block_slot = (piece % n).astype(jnp.int32)

    acts_t = acts.T.reshape(n, row_block, tokens_here)
    grad_tiles = jnp.moveaxis(grad_out.reshape(tokens_here, tiles_here, TILE), 1, 0)
    sends = 14 if n == 8 else 2 * (n - 1)
    in_vmem = pl.BlockSpec(memory_space=pltpu.VMEM)
    in_smem = pl.BlockSpec(memory_space=pltpu.SMEM)
    offload, sel_sum, norm = pl.pallas_call(
        functools.partial(gather_kernel, n),
        out_shape=(
            jax.ShapeDtypeStruct((capacity, row_block, TILE), jnp.bfloat16),
            jax.ShapeDtypeStruct((row_block, sel_count * TILE), jnp.float32),
            jax.ShapeDtypeStruct((tiles_here, 1, TILE), jnp.float32),
        ),
        in_specs=[in_smem] * 3 + [in_vmem] * 3,
        out_specs=(in_vmem,) * 3,
        scratch_shapes=[
            pltpu.VMEM((capacity, row_block, TILE), jnp.float32),
            pltpu.VMEM((n, tiles_here, 1, TILE), jnp.float32),
            pltpu.SemaphoreType.DMA((sends,)),
            pltpu.SemaphoreType.DMA((n - 1,)),
            pltpu.SemaphoreType.DMA((n - 1,)),
            pltpu.SemaphoreType.DMA((n - 1,)),
            pltpu.SemaphoreType.DMA((n - 1,)),
        ]
        + [pltpu.VMEM((n, row_block, tokens_here), jnp.bfloat16)] * (n - 1)
        + [pltpu.VMEM((tiles_here, tokens_here, TILE), jnp.bfloat16)] * (n - 1),
        compiler_params=pltpu.CompilerParams(
            collective_id=0, has_side_effects=True, vmem_limit_bytes=VMEM_LIMIT
        ),
    )(tile_slot, block_slot, selected_row, acts, acts_t, grad_tiles)
    new_sel = adam_update(sel_weight, sel_moment, sel_second, sel_sum)
    zero_half = jnp.zeros((), jnp.bfloat16)
    off_grad = jnp.where(filled[:, None, None], offload, zero_half).astype(jnp.float32)
    new_off = adam_update(
        off_weight, off_moment, off_second, off_grad.reshape(off_weight.shape)
    )
    return (norm.reshape(cols_here), *new_sel, *new_off)


def solution(mesh):
    placed = (
        P("dp", None),
        P("dp", "tensor"),
        P("tensor", None),
        P("tensor", None, None),
        P("dp", "tensor"),
        P("dp", "tensor"),
        P("dp", "tensor"),
        P("dp", "tensor", None, None, None),
        P("dp", "tensor", None, None, None),
        P("dp", "tensor", None, None, None),
    )
    return jax.shard_map(
        body,
        mesh=mesh,
        in_specs=placed,
        out_specs=(
            P("tensor"),
            P("dp", "tensor"),
            P("dp", "tensor"),
            P("dp", "tensor"),
            P("dp", "tensor", None, None, None),
            P("dp", "tensor", None, None, None),
            P("dp", "tensor", None, None, None),
        ),
        check_vma=False,
    )
```

```python
import functools

import jax
import jax.numpy as jnp
from jax import lax
from jax.experimental import pallas as pl
from jax.experimental.pallas import tpu as pltpu
from jax.sharding import PartitionSpec as P

TILE = 128
VMEM_LIMIT = 56 * 1024 * 1024


beta_one = 0.9
beta_two = 0.95
adam_eps = 1e-08
learn_rate = 0.01
decay_rate = 0.1
step_count = 10.0


def adam_update(weight, moment, second, grad):
    moment_new = beta_one * moment + (1.0 - beta_one) * grad
    second_new = beta_two * second + (1.0 - beta_two) * grad * grad
    first_fix = 1.0 - beta_one**step_count
    second_fix = 1.0 - beta_two**step_count
    update = moment_new / first_fix / (jnp.sqrt(second_new / second_fix) + adam_eps)
    return (weight - learn_rate * (update + decay_rate * weight), moment_new, second_new)


MESH = pl.DeviceIdType.MESH


def flip_bits(index, mask):
    result, bit = index, 1
    while bit <= mask:
        if mask & bit:
            result = result + bit * (1 - 2 * ((index // bit) % 2))
        bit *= 2
    return result


def gather_kernel(
    n,
    paired,
    tile_slot,
    block_slot,
    sel_tile,
    acts,
    acts_t,
    grad,
    offload,
    sel_sum,
    norm,
    total,
    squares,
    send_sem,
    recv_a,
    recv_z,
    recv_g,
    recv_e,
    send_q,
    recv_q,
    *held,
):
    held_a, held_g = (acts_t,) + held[: n - 1], (grad,) + held[n - 1 :]
    layer = lax.axis_index("tensor")
    half, cut = n // 2, grad.shape[0] * 3 // 4
    side = layer % 2
    parts = {
        "a": (held_a, pl.ds(side * half, half), recv_a),
        "z": (held_a, pl.ds((1 - side) * half, half), recv_z),
        "g": (held_g, pl.ds(0, cut), recv_g),
        "e": (held_g, pl.ds(cut, grad.shape[0] - cut), recv_e),
    }
    me = lax.axis_index("dp")
    capacity = offload.shape[0]
    sel_count = sel_tile.shape[0]
    rows_all = acts.shape[1]

    barrier = pltpu.get_barrier_semaphore()
    for mask in range(1, n):
        pl.semaphore_signal(
            barrier, inc=1, device_id={"dp": flip_bits(me, mask)}, device_id_type=MESH
        )
    if paired:
        pl.semaphore_signal(
            barrier, inc=1, device_id={"tensor": flip_bits(layer, 1)}, device_id_type=MESH
        )
    pl.semaphore_wait(barrier, n if paired else n - 1)

    started = []

    def part_of(kind, mask):
        slots, place, _ = parts[kind]
        return slots[mask].at[place]

    def copy_of(kind, mask, peer, number):
        there = mask ^ peer
        return pltpu.make_async_remote_copy(
            src_ref=part_of(kind, mask),
            dst_ref=part_of(kind, there),
            send_sem=send_sem.at[number],
            recv_sem=parts[kind][2].at[there - 1],
            device_id={"dp": flip_bits(me, peer)},
            device_id_type=MESH,
        )

    def send_across(mask):
        part = part_of("a", mask)
        copy = pltpu.make_async_remote_copy(
            src_ref=part,
            dst_ref=part,
            send_sem=send_sem.at[len(started)],
            recv_sem=recv_z.at[mask - 1],
            device_id={"tensor": flip_bits(layer, 1)},
            device_id_type=MESH,
        )
        copy.start()
        started.append(copy)

    def send(kind, mask, peer):
        copy = copy_of(kind, mask, peer, len(started))
        copy.start()
        started.append(copy)

    def arrived(kind, mask):
        copy_of(kind, 0, mask, 0).wait_recv()

    def square_columns():
        gram = jnp.dot(
            acts[...], acts_t[...].reshape(rows_all, -1), preferred_element_type=jnp.float32
        )
        high = gram.astype(jnp.bfloat16)
        rest = gram - high.astype(jnp.float32)
        middle = rest.astype(jnp.bfloat16)
        low = (rest - middle.astype(jnp.float32)).astype(jnp.bfloat16)

        @pl.loop(0, grad.shape[0])
        def _(tile):
            piece = grad[tile]
            product = jnp.dot(low, piece, preferred_element_type=jnp.float32)
            product += jnp.dot(middle, piece, preferred_element_type=jnp.float32)
            product += jnp.dot(high, piece, preferred_element_type=jnp.float32)
            squares[0, tile] = jnp.sum(
                piece.astype(jnp.float32) * product, axis=0, keepdims=True
            )

    def square_copy(mask):
        return pltpu.make_async_remote_copy(
            src_ref=squares.at[0],
            dst_ref=squares.at[mask],
            send_sem=send_q.at[mask - 1],
            recv_sem=recv_q.at[mask - 1],
            device_id={"dp": flip_bits(me, mask)},
            device_id_type=MESH,
        )

    def add_blocks(masks, first, last):
        def product(mask, block, tile):
            return jnp.dot(
                held_a[mask][block], held_g[mask][tile], preferred_element_type=jnp.float32
            )

        @pl.loop(0, capacity)
        def _(slot):
            block, tile = block_slot[slot], tile_slot[slot]
            value = None if first else total[slot]
            for mask in masks:
                part = product(mask, block, tile)
                part = part.astype(jnp.bfloat16).astype(jnp.float32)
                value = part if value is None else value + part
            if last:
                offload[slot] = value.astype(jnp.bfloat16)
            else:
                total[slot] = value

        for i in range(sel_count):
            tile = sel_tile[i]
            place = pl.ds(i * TILE, TILE)
            value = None if first else sel_sum[:, place]
            for mask in masks:
                part = product(mask, me, tile)
                value = part if value is None else value + part
            sel_sum[:, place] = value

    def relay(kinds, mask):
        for kind in kinds:
            arrived(kind, mask)
            send(kind, mask, 1)

    def complete(mask):
        for kind in parts:
            arrived(kind, mask)

    def send_squares():
        for mask in range(1, n):
            square_copy(mask).start()

    if paired:
        core, near, far = 1, 2, 4
        both = near ^ far
        send("a", 0, near)
        send("a", 0, far)
        send("g", 0, near)
        send("g", 0, far)
        send("e", 0, far)
        for kind in parts:
            send(kind, 0, core)
        square_columns()
        arrived("a", far)
        send("a", far, near)
        send("e", 0, near)
        send_across(far)
        send("a", far, core)
        arrived("a", near)
        send_across(near)
        send("a", near, core)
        complete(core)
        add_blocks((0, core), True, False)
        send_squares()
        relay("z", far)
        arrived("g", near)
        send("g", near, far)
        send("g", near, core)
        arrived("e", far)
        send("e", far, near)
        send("e", far, core)
        relay("g", far)
        add_blocks((far,), False, False)
        arrived("a", both)
        send_across(both)
        send("a", both, core)
        relay("z", near)
        complete(far ^ core)
        add_blocks((far ^ core,), False, False)
        relay("e", near)
        complete(near ^ core)
        add_blocks((near, near ^ core), False, False)
        relay("gez", both)
        complete(both ^ core)
        add_blocks((both, both ^ core), False, True)
    else:
        for mask in range(1, n):
            for kind in parts:
                send(kind, 0, mask)
        square_columns()
        add_blocks((0,), True, False)
        send_squares()
        for mask in range(1, n):
            complete(mask)
            add_blocks((mask,), False, mask == n - 1)

    whole = squares[0]
    for mask in range(1, n):
        square_copy(mask).wait_recv()
        whole = whole + squares[mask]
    norm[...] = jnp.sqrt(whole)
    for copy in started:
        copy.wait_send()
    for mask in range(1, n):
        square_copy(mask).wait_send()


def body(
    acts,
    grad_out,
    selected,
    owner,
    sel_weight,
    sel_moment,
    sel_second,
    off_weight,
    off_moment,
    off_second,
):
    n = lax.axis_size("dp")
    tokens_here, rows_all = acts.shape
    cols_here = grad_out.shape[1]
    tiles_here = cols_here // TILE
    sel_count = selected.shape[1]
    rest_count = tiles_here - sel_count
    row_block = rows_all // n
    capacity = off_weight.shape[2]
    piece_count = rest_count * n
    selected_row = selected[0]
    owner_row = owner[0, :, 0]
    mine = (owner_row == lax.axis_index("dp")).astype(jnp.int32)
    pieces = jnp.arange(piece_count, dtype=jnp.int32)
    before = jnp.sum(mine[None, :] * (pieces[:, None] > pieces[None, :]), axis=1)
    taken = mine[None, :] * (before[None, :] == jnp.arange(capacity)[:, None])
    piece = jnp.sum(taken * pieces[None, :], axis=1)
    filled = jnp.sum(taken, axis=1) > 0
    order = piece // n
    tiles = jnp.arange(tiles_here, dtype=jnp.int32)
    free = 1 - jnp.any(tiles[:, None] == selected_row[None, :], axis=1).astype(jnp.int32)
    rank = jnp.sum(free[None, :] * (tiles[:, None] > tiles[None, :]), axis=1)
    named = free[None, :] * (rank[None, :] == order[:, None])
    tile_slot = jnp.sum(named * tiles[None, :], axis=1).astype(jnp.int32)
    block_slot = (piece % n).astype(jnp.int32)

    acts_t = acts.T.reshape(n, row_block, tokens_here)
    grad_tiles = jnp.moveaxis(grad_out.reshape(tokens_here, tiles_here, TILE), 1, 0)
    paired = n == 8 and lax.axis_size("tensor") % 2 == 0
    sends = 28 if paired else 4 * (n - 1)
    in_vmem = pl.BlockSpec(memory_space=pltpu.VMEM)
    in_smem = pl.BlockSpec(memory_space=pltpu.SMEM)
    offload, sel_sum, norm = pl.pallas_call(
        functools.partial(gather_kernel, n, paired),
        out_shape=(
            jax.ShapeDtypeStruct((capacity, row_block, TILE), jnp.bfloat16),
            jax.ShapeDtypeStruct((row_block, sel_count * TILE), jnp.float32),
            jax.ShapeDtypeStruct((tiles_here, 1, TILE), jnp.float32),
        ),
        in_specs=[in_smem] * 3 + [in_vmem] * 3,
        out_specs=(in_vmem,) * 3,
        scratch_shapes=[
            pltpu.VMEM((capacity, row_block, TILE), jnp.float32),
            pltpu.VMEM((n, tiles_here, 1, TILE), jnp.float32),
            pltpu.SemaphoreType.DMA((sends,)),
            pltpu.SemaphoreType.DMA((n - 1,)),
            pltpu.SemaphoreType.DMA((n - 1,)),
            pltpu.SemaphoreType.DMA((n - 1,)),
            pltpu.SemaphoreType.DMA((n - 1,)),
            pltpu.SemaphoreType.DMA((n - 1,)),
            pltpu.SemaphoreType.DMA((n - 1,)),
        ]
        + [pltpu.VMEM((n, row_block, tokens_here), jnp.bfloat16)] * (n - 1)
        + [pltpu.VMEM((tiles_here, tokens_here, TILE), jnp.bfloat16)] * (n - 1),
        compiler_params=pltpu.CompilerParams(
            collective_id=0, has_side_effects=True, vmem_limit_bytes=VMEM_LIMIT
        ),
    )(tile_slot, block_slot, selected_row, acts, acts_t, grad_tiles)
    new_sel = adam_update(sel_weight, sel_moment, sel_second, sel_sum)
    zero_half = jnp.zeros((), jnp.bfloat16)
    off_grad = jnp.where(filled[:, None, None], offload, zero_half).astype(jnp.float32)
    new_off = adam_update(
        off_weight, off_moment, off_second, off_grad.reshape(off_weight.shape)
    )
    return (norm.reshape(cols_here), *new_sel, *new_off)


def solution(mesh):
    placed = (
        P("dp", None),
        P("dp", "tensor"),
        P("tensor", None),
        P("tensor", None, None),
        P("dp", "tensor"),
        P("dp", "tensor"),
        P("dp", "tensor"),
        P("dp", "tensor", None, None, None),
        P("dp", "tensor", None, None, None),
        P("dp", "tensor", None, None, None),
    )
    return jax.shard_map(
        body,
        mesh=mesh,
        in_specs=placed,
        out_specs=(
            P("tensor"),
            P("dp", "tensor"),
            P("dp", "tensor"),
            P("dp", "tensor"),
            P("dp", "tensor", None, None, None),
            P("dp", "tensor", None, None, None),
            P("dp", "tensor", None, None, None),
        ),
        check_vma=False,
    )
```
